32 devices in a mesh: rows: 8 (over z, y), rank: 4 (over x, core).
Axes of the slice: x: 2, y: 2, z: 4, core: 2. Of those that a mesh axis runs over, the one named last changes fastest.
Arguments:
- left_factor: bfloat16 [128, 16384], P(None, 'rows'), may hold values from -8 to 8
- right_factor: bfloat16 [128, 16384], P(None, 'rows'), may hold values from -8 to 8
- left_plan: float32 [256, 16384], P('rank', 'rows'), may hold values from 0.0068 to 147, as said below
- right_plan: float32 [256, 16384], P('rank', 'rows'), may hold values from 0.0068 to 147, as said below
- log_inner: float32 [256], P('rank'), may hold values from -1 to 1
- left_mass: float32 [16384], P('rows'), may hold values from 32 to 1024, as said below
- right_mass: float32 [16384], P('rows'), may hold values from 32 to 1024, as said below
Outputs:
- new_left: float32 [256, 16384], P('rank', 'rows')
- new_right: float32 [256, 16384], P('rank', 'rows')
- new_log_inner: float32 [256], P('rank')
The draws below stay inside these ranges and needn't reach their ends.
Inputs may be any that keep to these rules, and one draw needn't show every extreme that they name: `left_plan`: positive entries. `right_plan`: positive entries. `left_mass`: positive point masses. `right_mass`: positive point masses.
All inputs are finite; a program needn't handle non-finite values. Where the reference program divides by a largest or mean magnitude, that divisor is 1e-20 or more.
Results may differ from the reference program's by a relative error of at most 0.00045.
Values sent between devices are 32-bit elements; how exact they have to be, the bound alone decides.
A program may use at most 64 MiB of HBM per device.

```python
import math
import jax
import jax.numpy as jnp
from jax import lax

DC = 128
RANK = 256
ROWS_DEV = 2048
ITERS = 3
POINTS = 16384


def draw_masses(key):
    blocks = POINTS // ROWS_DEV
    level = jnp.exp(jax.random.uniform(jax.random.fold_in(key, 1), (blocks, 1), jnp.float32, math.log(32.0), math.log(512.0)))
    factor = jax.random.uniform(jax.random.fold_in(key, 2), (blocks, ROWS_DEV), jnp.float32, 1.0, 2.0)
    return (level * factor).reshape(POINTS)


def draw_left_mass(key, part):
    return draw_masses(jax.random.fold_in(key, 11))


def draw_right_mass(key, part):
    return draw_masses(jax.random.fold_in(key, 23))


def draw_points(key, salt):
    blocks = POINTS // ROWS_DEV
    inner_key = jax.random.fold_in(key, salt)
    offset = jax.random.uniform(jax.random.fold_in(inner_key, 5), (blocks, 1), jnp.float32, -1.25, 1.25)
    offset = jnp.broadcast_to(offset, (blocks, ROWS_DEV)).reshape(1, POINTS)
    noise = jax.random.truncated_normal(jax.random.fold_in(inner_key, 2), -2.75, 2.75, (DC, POINTS), jnp.float32)
    return jnp.clip(noise + offset, -4.0, 4.0)


def draw_directions(key):
    return jax.random.normal(jax.random.fold_in(key, 307), (DC, RANK), jnp.float32) / math.sqrt(DC)


def draw_plan(key, salt):
    blocks = POINTS // ROWS_DEV
    inner_key = jax.random.fold_in(key, salt)
    points = draw_points(key, salt)
    directions = draw_directions(key)
    align = jnp.dot(directions.T, points, precision=lax.Precision.HIGHEST)
    align = jnp.clip(align, -3.0, 3.0).reshape(RANK, blocks, ROWS_DEV)
    strength = jax.random.uniform(jax.random.fold_in(inner_key, 3), (1, blocks, 1), jnp.float32, 0.4, 1.2)
    leaning = jnp.exp(strength * align).reshape(RANK, POINTS)
    base = jnp.exp(jax.random.uniform(jax.random.fold_in(inner_key, 4), (RANK, POINTS), jnp.float32, math.log(0.25), math.log(4.0)))
    return base * leaning


def draw_left_factor(key, part):
    return (2.0 * draw_points(key, 101)).astype(jnp.bfloat16)


def draw_right_factor(key, part):
    return (2.0 * draw_points(key, 202)).astype(jnp.bfloat16)


def draw_left_plan(key, part):
    return draw_plan(key, 101)


def draw_right_plan(key, part):
    return draw_plan(key, 202)


def shard_levels(key, extent, split, low, top_value):
    def one(position, parts):
        heights = jax.random.uniform(jax.random.fold_in(jax.random.fold_in(key, 6), position), (parts,), jnp.float32, low / len(split), top_value / len(split))
        return jnp.repeat(jnp.exp(heights), extent[position] // parts).reshape((-1,) + (1,) * (len(extent) - position - 1))

    loudness = one(*split[0])
    for cut in split[1:]:
        loudness = loudness * one(*cut)
    return loudness


def setup_inputs(seed: int = 0) -> dict:
    keys = jax.random.split(jax.random.key(seed), 8)
    left_factor = draw_left_factor(jax.random.fold_in(keys[7], 71), 0)
    right_factor = draw_right_factor(jax.random.fold_in(keys[7], 71), 0)
    left_plan = draw_left_plan(jax.random.fold_in(keys[7], 71), 0)
    right_plan = draw_right_plan(jax.random.fold_in(keys[7], 71), 0)
    log_inner = jnp.clip(jax.random.uniform(keys[4], (RANK,), jnp.float32, -1.0, 1.0) * shard_levels(keys[4], (RANK,), ((0, 4),), -0.4, 0.0), -1.0, 1.0)
    left_mass = draw_left_mass(jax.random.fold_in(keys[7], 71), 0)
    right_mass = draw_right_mass(jax.random.fold_in(keys[7], 71), 0)
    return {"left_factor": left_factor, "right_factor": right_factor, "left_plan": left_plan, "right_plan": right_plan, "log_inner": log_inner, "left_mass": left_mass, "right_mass": right_mass}


def balance(inner_mass, col_scale_left, col_total_left, col_scale_right, col_total_right):
    mixed = jnp.log(inner_mass) + jnp.log(col_scale_left * col_total_left) + jnp.log(col_scale_right * col_total_right)
    inner_mass = jnp.exp(mixed / 3.0)
    return inner_mass, inner_mass / col_total_left, inner_mass / col_total_right


def reference(left_factor, right_factor, left_plan, right_plan, log_inner, left_mass, right_mass):
    precise = lax.Precision.HIGHEST
    total_left = jnp.sum(left_mass)
    total_right = jnp.sum(right_mass)
    inner_mass = (total_left / RANK) * jnp.exp(log_inner)
    left_round = left_plan.astype(jnp.bfloat16)
    right_round = right_plan.astype(jnp.bfloat16)
    proj_right = jnp.dot(right_factor, right_round.T, preferred_element_type=jnp.float32)
    proj_left = jnp.dot(left_factor, left_round.T, preferred_element_type=jnp.float32)
    scaled_right = (proj_right / inner_mass[None, :]).astype(jnp.bfloat16)
    scaled_left = (proj_left / inner_mass[None, :]).astype(jnp.bfloat16)
    grad_left = jnp.dot(scaled_right.T, left_factor, preferred_element_type=jnp.float32)
    grad_right = jnp.dot(scaled_left.T, right_factor, preferred_element_type=jnp.float32)
    pairing = jnp.sum(left_round.astype(jnp.float32) * grad_left, axis=1)
    grad_inner = -pairing / inner_mass
    largest = jnp.maximum(jnp.maximum(jnp.max(jnp.abs(grad_left)), jnp.max(jnp.abs(grad_right))), jnp.max(jnp.abs(grad_inner)))
    step_size = 5.0 / jnp.maximum(largest, 0.25)
    tilted_left = left_plan * jnp.exp(-step_size * grad_left)
    tilted_right = right_plan * jnp.exp(-step_size * grad_right)
    inner_mass = inner_mass * jnp.exp(-step_size * grad_inner)
    right_norm = right_mass * (total_left / total_right)
    col_scale_left = jnp.ones((RANK,), jnp.float32)
    col_scale_right = jnp.ones((RANK,), jnp.float32)
    row_scale_left = left_mass
    row_scale_right = right_norm
    for repeat in range(ITERS):
        row_scale_left = left_mass / jnp.dot(col_scale_left, tilted_left, precision=precise)
        row_scale_right = right_norm / jnp.dot(col_scale_right, tilted_right, precision=precise)
        col_total_left = jnp.dot(tilted_left, row_scale_left, precision=precise)
        col_total_right = jnp.dot(tilted_right, row_scale_right, precision=precise)
        inner_mass, col_scale_left, col_scale_right = balance(inner_mass, col_scale_left, col_total_left, col_scale_right, col_total_right)
    new_left = row_scale_left[None, :] * tilted_left * col_scale_left[:, None]
    new_right = row_scale_right[None, :] * tilted_right * col_scale_right[:, None]
    new_log_inner = jnp.log(inner_mass) - jnp.log(total_left / RANK)
    return new_left, new_right, new_log_inner
```

```python
import functools

import jax
import jax.numpy as jnp
from jax import lax
from jax.experimental import pallas as pl
from jax.experimental.pallas import tpu as pltpu
from jax.sharding import PartitionSpec as P

ITERS = 3
LANES = 128
UNROLL = 32
MESH = pl.DeviceIdType.MESH


def each(start, stop, body):
    if stop - start <= UNROLL:
        for index in range(start, stop):
            body(index)
    else:
        pl.loop(start, stop)(body)


def to_columns(row):
    return jnp.broadcast_to(row, (LANES, row.shape[1])).T


def kernel(
    n_rows, n_rank,
    lf_hbm, rf_hbm, lp_hbm, rp_hbm, log_ref, lm_ref, rm_ref,
    tl_hbm, tr_hbm, scale_ref, col_ref, log_out,
    lf, rf, lp, rp, tilt, log_row,
    part, parts, chunk, proj, totals, tops, sums, cols,
    in_sems, out_sems, part_send, part_recv, tot_send, tot_recv, proj_send, proj_recv,
    top_send, top_recv, sum_send, sum_recv, col_send, col_recv,
):
    row, rank = lax.axis_index("rows"), lax.axis_index("rank")
    everyone = n_rows * n_rank
    flat = row * n_rank + rank
    k, points = lp.shape
    ranks = k * n_rank
    tiles = points // LANES

    barrier = pltpu.get_barrier_semaphore()

    def place(other):
        return (other // n_rank, other % n_rank)

    def greet(step):
        pl.semaphore_signal(
            barrier, inc=1, device_id=place((flat + step) % everyone), device_id_type=MESH
        )

    each(1, everyone, greet)
    loads = []
    for index, (source, target) in enumerate(((lp_hbm, lp), (lf_hbm, lf), (rp_hbm, rp), (rf_hbm, rf))):
        load = pltpu.make_async_copy(source, target, in_sems.at[index])
        load.start()
        loads.append(load)

    def row_peer(step):
        return ((row + step) % n_rows, rank)

    def rank_peer(step):
        return (row, (rank + step) % n_rank)

    def flat_peer(step):
        return place((flat + step) % everyone)

    def copy(source, target, send, recv, device):
        return pltpu.make_async_remote_copy(
            src_ref=source, dst_ref=target, send_sem=send, recv_sem=recv,
            device_id=device, device_id_type=MESH,
        )

    def tile(ref, j):
        return ref[:, j * LANES : (j + 1) * LANES]

    for side, mass in enumerate((lm_ref, rm_ref)):
        total = tile(mass, 0)
        for j in range(1, tiles):
            total = total + tile(mass, j)
        totals[row, side : side + 1, :] = total
    log_row[:, :k] = log_ref[...]
    log_row[:, k:] = log_ref[...]

    def product(plan, factor):
        return lax.dot_general(
            plan[...].astype(jnp.bfloat16), factor[...], (((1,), (1,)), ((), ())),
            preferred_element_type=jnp.float32,
        )

    loads[0].wait()
    loads[1].wait()
    both = [product(lp, lf)]
    loads[2].wait()
    loads[3].wait()
    both.append(product(rp, rf))
    local = jnp.concatenate(both, axis=0)
    part[...] = local.reshape(part.shape)
    pl.semaphore_wait(barrier, everyone - 1)

    def part_copy(step):
        peer = (row + step) % n_rows
        return copy(part.at[peer], parts.at[row], part_send.at[step], part_recv.at[step], row_peer(step))

    def tot_copy(step):
        return copy(totals.at[row], totals.at[row], tot_send.at[step], tot_recv.at[step], row_peer(step))

    def proj_copy(step):
        return copy(proj.at[row], proj.at[row], proj_send.at[step], proj_recv.at[step], row_peer(step))

    each(1, n_rows, lambda step: part_copy(step).start())
    each(1, n_rows, lambda step: tot_copy(step).start())
    parts[row] = part[row]
    each(1, n_rows, lambda step: part_copy(step).wait_recv())
    proj[row] = jnp.sum(parts[...], axis=0)
    each(1, n_rows, lambda step: proj_copy(step).start())

    each(1, n_rows, lambda step: tot_copy(step).wait_recv())
    total = jnp.sum(jnp.sum(totals[...], axis=0), axis=1, keepdims=True)
    total_left, total_right = total[0:1], total[1:2]
    mean = total_left / ranks
    inner = mean * jnp.exp(log_row[...])
    inner_columns = to_columns(inner)
    norm = total_left / total_right
    mass_left = lm_ref[...]
    mass_right = rm_ref[...] * norm

    each(1, n_rows, lambda step: proj_copy(step).wait_recv())
    sums_all = proj[...].reshape(2 * k, LANES)
    scaled = (sums_all / inner_columns).astype(jnp.bfloat16)
    grads = []
    for scale, factor in ((scaled[k:], lf), (scaled[:k], rf)):
        grads.append(
            lax.dot_general(
                scale, factor[...], (((1,), (0,)), ((), ())), preferred_element_type=jnp.float32
            )
        )
    pair = scaled[k:].astype(jnp.float32) * sums_all[:k]
    pairing = jnp.sum(jnp.concatenate([pair, pair], axis=0).T, axis=0, keepdims=True)
    grad_inner = -pairing / inner
    peak = jnp.maximum(jnp.abs(grads[0]), jnp.abs(grads[1]))
    peak = jnp.max(peak, axis=0, keepdims=True)
    top = jnp.abs(grad_inner)
    for j in range(tiles):
        top = jnp.maximum(top, peak[:, j * LANES : (j + 1) * LANES])
    tops[flat] = top

    def top_copy(step):
        return copy(tops.at[flat], tops.at[flat], top_send.at[step], top_recv.at[step], flat_peer(step))

    each(1, everyone, lambda step: top_copy(step).start())
    each(1, everyone, lambda step: top_copy(step).wait_recv())
    largest = jnp.max(jnp.max(tops[...], axis=0), axis=1, keepdims=True)
    size = 5.0 / jnp.maximum(largest, 0.25)
    tilt[0] = lp[...] * jnp.exp(-size * grads[0])
    tilt[1] = rp[...] * jnp.exp(-size * grads[1])
    stores = []
    for side, target in enumerate((tl_hbm, tr_hbm)):
        store = pltpu.make_async_copy(tilt.at[side], target, out_sems.at[side])
        store.start()
        stores.append(store)
    log_inner = jnp.log(inner * jnp.exp(-size * grad_inner))
    col = jnp.ones_like(inner)
    columns = None

    for repeat in range(ITERS):
        def sum_copy(step):
            return copy(
                sums.at[repeat, rank], sums.at[repeat, rank],
                sum_send.at[repeat, step], sum_recv.at[repeat, step], rank_peer(step),
            )

        def col_copy(step):
            return copy(
                cols.at[repeat, row], cols.at[repeat, row],
                col_send.at[repeat, step], col_recv.at[repeat, step], row_peer(step),
            )

        for side in range(2):
            for j in range(tiles):
                lanes = slice(j * LANES, (j + 1) * LANES)
                block = tilt[side, :, lanes]
                if columns is not None:
                    block = block * columns[side * k : (side + 1) * k]
                sums[repeat, rank, side : side + 1, lanes] = jnp.sum(block, axis=0, keepdims=True)
        each(1, n_rank, lambda step: sum_copy(step).start())
        each(1, n_rank, lambda step: sum_copy(step).wait_recv())
        weight = jnp.sum(sums[repeat], axis=0)
        scales = (mass_left / weight[0:1], mass_right / weight[1:2])
        partial = []
        for side in range(2):
            acc = None
            for j in range(tiles):
                lanes = slice(j * LANES, (j + 1) * LANES)
                term = tilt[side, :, lanes] * scales[side][:, lanes]
                acc = term if acc is None else acc + term
            partial.append(acc)
        cols[repeat, row] = jnp.sum(jnp.concatenate(partial, axis=0).T, axis=0, keepdims=True)
        each(1, n_rows, lambda step: col_copy(step).start())
        if repeat == ITERS - 1:
            scale_ref[0:1, :] = scales[0]
            scale_ref[1:2, :] = scales[1]
        each(1, n_rows, lambda step: col_copy(step).wait_recv())
        total_col = jnp.sum(cols[repeat], axis=0)
        own = jnp.log(col * total_col)
        log_inner = (log_inner + own + pltpu.roll(own, k, 1)) / 3.0
        col = jnp.exp(log_inner) / total_col
        if repeat < ITERS - 1:
            columns = to_columns(col)
        each(1, n_rank, lambda step: sum_copy(step).wait_send())
        each(1, n_rows, lambda step: col_copy(step).wait_send())

    col_ref[...] = col
    log_out[...] = log_inner - jnp.log(mean)
    each(1, n_rows, lambda step: part_copy(step).wait_send())
    each(1, n_rows, lambda step: tot_copy(step).wait_send())
    each(1, n_rows, lambda step: proj_copy(step).wait_send())
    each(1, everyone, lambda step: top_copy(step).wait_send())
    for store in stores:
        store.wait()


def solution(mesh):
    n_rows, n_rank = mesh.shape["rows"], mesh.shape["rank"]
    everyone = n_rows * n_rank

    def per_device(left_factor, right_factor, left_plan, right_plan, log_inner, left_mass, right_mass):
        k, points = left_plan.shape
        depth = left_factor.shape[0]
        lines = 2 * k // n_rows
        f32 = jnp.float32
        whole = pl.BlockSpec(memory_space=pl.ANY)
        near = pl.BlockSpec(memory_space=pltpu.VMEM)
        dma = pltpu.SemaphoreType.DMA
        tilted_left, tilted_right, row_scale, col_scale, new_log = pl.pallas_call(
            functools.partial(kernel, n_rows, n_rank),
            out_shape=(
                jax.ShapeDtypeStruct((k, points), f32),
                jax.ShapeDtypeStruct((k, points), f32),
                jax.ShapeDtypeStruct((2, points), f32),
                jax.ShapeDtypeStruct((1, 2 * k), f32),
                jax.ShapeDtypeStruct((1, 2 * k), f32),
            ),
            in_specs=[whole] * 4 + [near] * 3,
            out_specs=(whole, whole, near, near, near),
            scratch_shapes=[
                pltpu.VMEM((depth, points), jnp.bfloat16),
                pltpu.VMEM((depth, points), jnp.bfloat16),
                pltpu.VMEM((k, points), f32),
                pltpu.VMEM((k, points), f32),
                pltpu.VMEM((2, k, points), f32),
                pltpu.VMEM((1, 2 * k), f32),
                pltpu.VMEM((n_rows, lines, depth), f32),
                pltpu.VMEM((n_rows, lines, depth), f32),
                pltpu.VMEM((lines, depth), f32),
                pltpu.VMEM((n_rows, lines, depth), f32),
                pltpu.VMEM((n_rows, 2, LANES), f32),
                pltpu.VMEM((everyone, 1, LANES), f32),
                pltpu.VMEM((ITERS, n_rank, 2, points), f32),
                pltpu.VMEM((ITERS, n_rows, 1, 2 * k), f32),
                dma((4,)),
                dma((2,)),
                dma((n_rows,)),
                dma((n_rows,)),
                dma((n_rows,)),
                dma((n_rows,)),
                dma((n_rows,)),
                dma((n_rows,)),
                dma((everyone,)),
                dma((everyone,)),
                dma((ITERS, n_rank)),
                dma((ITERS, n_rank)),
                dma((ITERS, n_rows)),
                dma((ITERS, n_rows)),
            ],
            compiler_params=pltpu.CompilerParams(collective_id=0, has_side_effects=True),
        )(
            left_factor, right_factor, left_plan, right_plan,
            log_inner[None, :], left_mass[None, :], right_mass[None, :],
        )
        new_left = row_scale[0][None, :] * tilted_left * col_scale[0, :k][:, None]
        new_right = row_scale[1][None, :] * tilted_right * col_scale[0, k:][:, None]
        return new_left, new_right, new_log[0, :k]

    in_specs = (
        P(None, "rows"),
        P(None, "rows"),
        P("rank", "rows"),
        P("rank", "rows"),
        P("rank"),
        P("rows"),
        P("rows"),
    )
    out_specs = (P("rank", "rows"), P("rank", "rows"), P("rank"))
    return jax.shard_map(
        per_device, mesh=mesh, in_specs=in_specs, out_specs=out_specs, check_vma=False
    )
```
